32 devices in a mesh: node: 8 (over z, x), chan: 4 (over y, core).
Axes of the slice: x: 2, y: 2, z: 4, core: 2. Of those that a mesh axis runs over, the one named last changes fastest.
Arguments:
- nodes: bfloat16 [1024, 512], P('node'), may hold values from -6 to 6
- edges: bfloat16 [3072, 512], P('node'), may hold values from -6 to 6
- grad_nodes_in: bfloat16 [1024, 512], P('node'), may hold values from -6 to 6
- grad_edges_in: bfloat16 [3072, 512], P('node'), may hold values from -6 to 6
- edge_in_weight: bfloat16 [1536, 512], P(None, 'chan'), may hold values from -0.15625 to 0.15625
- edge_bias: float32 [512], P('chan'), may hold values from -4 to 4
- edge_out_weight: bfloat16 [512, 512], P('chan'), may hold values from -0.25 to 0.25
- node_in_weight: bfloat16 [1024, 512], P(None, 'chan'), may hold values from -0.1875 to 0.1875
- node_bias: float32 [512], P('chan'), may hold values from -4 to 4
- node_out_weight: bfloat16 [512, 512], P('chan'), may hold values from -0.25 to 0.25
- senders: int32 [3072], P('node'), may hold values from 0 to 135
- receivers: int32 [3072], P('node'), may hold values from 0 to 127, as said below
- valid_counts: int32 [24], P('node'), may hold values from 1 to 128
- send_list: int32 [64, 1], P('node'), may hold values from 0 to 127
Outputs:
- grad_nodes: bfloat16 [1024, 512], P('node', 'chan')
- grad_edges: bfloat16 [3072, 512], P('node', 'chan')
- grad_edge_in: float32 [1536, 512], P('node', 'chan')
- grad_edge_out: float32 [512, 512], P('chan', 'node')
- grad_node_in: float32 [1024, 512], P('node', 'chan')
- grad_node_out: float32 [512, 512], P('chan', 'node')
The draws below stay inside these ranges and needn't reach their ends.
Inputs may be any that keep to these rules, and one draw needn't show every extreme that they name: `senders`: below 128: a node of the slot's own owner; otherwise 128 + p + j, the j-th node that owner p sends to the slot's owner. `receivers`: A node number on the slot's owner, nondecreasing within each owner's 384 slots. `valid_counts`: the live slots of a block are its first ones. `send_list`: row p * 8 + q holds node numbers of owner p that owner q reads.
All inputs are finite; a program needn't handle non-finite values.
Results may differ from the reference program's by a relative error of at most 0.011.
Values may be sent and summed in bfloat16 or wider, within the bound.
No kernel may reach another device: no remote copies, remote signals or barrier semaphores. Data moves between devices by JAX's collectives and lax.ppermute only.
A program may use at most 64 MiB of HBM per device.

```python
import jax
import jax.numpy as jnp
from jax import lax

D = 512
H = 512
N_DEV = 128
E_DEV = 384
BLOCK = 128
SLOT = 1
OWNERS = 8
HALO = 8
NODES = 1024
EDGES = 3072


def draw_receivers(key, part):
    values = jax.random.randint(key, (OWNERS, E_DEV), 0, N_DEV)
    return jnp.sort(values, axis=1).reshape(-1).astype(jnp.int32)


def plant(drawn, rng, least, high):
    extent = drawn.shape
    spot = [jax.random.randint(jax.random.fold_in(rng, axis), (), 0, extent[axis]) for axis in range(len(extent))]
    drawn = drawn.at[tuple(spot)].set(least)
    longest = extent.index(max(extent))
    spot[longest] = (spot[longest] + 1) % extent[longest]
    return drawn.at[tuple(spot)].set(high)


def level_of(key, shape, cuts, least, high):
    factor_of = 1.0
    for dim, blocks in cuts:
        heights = jax.random.uniform(jax.random.fold_in(jax.random.fold_in(key, 6), dim), (blocks,), jnp.float32, least / len(cuts), high / len(cuts))
        factor_of = factor_of * jnp.repeat(jnp.exp(heights), shape[dim] // blocks).reshape((-1,) + (1,) * (len(shape) - 1 - dim))
    return factor_of


def noise(stream_key, extent, deviation, limit, shards=(), kind=jnp.bfloat16):
    values = deviation * jax.random.normal(stream_key, extent, jnp.float32)
    if shards:
        values = values * level_of(stream_key, extent, shards, -0.22, 0.18)
    return jnp.clip(values, -limit, limit).astype(kind)


def setup_inputs(seed: int = 0) -> dict:
    seeds = jax.random.split(jax.random.key(seed), 15)
    nodes = noise(seeds[0], (NODES, D), 1.0, 6.0, ((0, 8),))
    edges = noise(seeds[1], (EDGES, D), 1.0, 6.0, ((0, 8),))
    grad_nodes_in = noise(seeds[2], (NODES, D), 1.0, 6.0, ((0, 8),))
    grad_edges_in = noise(seeds[3], (EDGES, D), 1.0, 6.0, ((0, 8),))
    edge_in_weight = noise(seeds[4], (3 * D, H), (3 * D) ** -0.5, 0.15625, ((1, 4),))
    edge_bias = noise(seeds[5], (H,), 1.0, 4.0, ((0, 4),), jnp.float32)
    edge_out_weight = noise(seeds[6], (H, D), H ** -0.5, 0.25, ((0, 4),))
    node_in_weight = noise(seeds[7], (2 * D, H), (2 * D) ** -0.5, 0.1875, ((1, 4),))
    node_bias = noise(seeds[8], (H,), 1.0, 4.0, ((0, 4),), jnp.float32)
    node_out_weight = noise(seeds[9], (H, D), H ** -0.5, 0.25, ((0, 4),))
    senders = plant(jax.random.randint(seeds[10], (EDGES,), 0, N_DEV + HALO), jax.random.fold_in(seeds[10], 1), 0, (N_DEV + HALO) - 1).astype(jnp.int32)
    receivers = draw_receivers(jax.random.fold_in(seeds[14], 71), 0)
    valid_counts = plant(jax.random.randint(seeds[12], (EDGES // BLOCK,), 1, BLOCK + 1), jax.random.fold_in(seeds[12], 1), 1, BLOCK).astype(jnp.int32)
    send_list = plant(jax.random.randint(seeds[13], (OWNERS * OWNERS, SLOT), 0, N_DEV), jax.random.fold_in(seeds[13], 1), 0, N_DEV - 1).astype(jnp.int32)
    return dict(nodes=nodes, edges=edges, grad_nodes_in=grad_nodes_in, grad_edges_in=grad_edges_in, edge_in_weight=edge_in_weight, edge_bias=edge_bias, edge_out_weight=edge_out_weight, node_in_weight=node_in_weight, node_bias=node_bias, node_out_weight=node_out_weight, senders=senders, receivers=receivers, valid_counts=valid_counts, send_list=send_list)


def silu_parts(preact):
    logistic = jax.nn.sigmoid(preact)
    return preact * logistic, logistic * (1.0 + preact * (1.0 - logistic))


def contract(left_mat, right_mat, left_dim, right_dim):
    return lax.dot_general(left_mat, right_mat, (((left_dim,), (right_dim,)), ((), ())), preferred_element_type=jnp.float32)


def reference(nodes, edges, grad_nodes_in, grad_edges_in, edge_in_weight, edge_bias, edge_out_weight, node_in_weight, node_bias, node_out_weight, senders, receivers, valid_counts, send_list):
    owner_ids = jnp.arange(EDGES, dtype=jnp.int32) // E_DEV
    offset = jnp.maximum(senders - N_DEV, 0).astype(jnp.int32)
    peer_ids = offset // SLOT
    slot_ids = offset % SLOT
    remote = (send_list[peer_ids * OWNERS + owner_ids, slot_ids] + peer_ids * N_DEV).astype(jnp.int32)
    sender_rows = jnp.where(senders < N_DEV, owner_ids * N_DEV + senders, remote).astype(jnp.int32)
    receiver_rows = (owner_ids * N_DEV + receivers).astype(jnp.int32)
    position = jnp.arange(EDGES, dtype=jnp.int32) % BLOCK
    live_mask = (position < jnp.repeat(valid_counts, BLOCK)).astype(jnp.float32)[:, None]
    stacked = jnp.concatenate([edges, nodes[sender_rows], nodes[receiver_rows]], axis=1)
    edge_pre = jnp.dot(stacked, edge_in_weight, preferred_element_type=jnp.float32) + edge_bias
    edge_act, edge_slope = silu_parts(edge_pre)
    hidden = (edge_act * live_mask).astype(jnp.bfloat16)
    hidden_sums = jax.ops.segment_sum(hidden.astype(jnp.float32), receiver_rows, num_segments=NODES).astype(jnp.bfloat16)
    aggregate = jnp.dot(hidden_sums, edge_out_weight, preferred_element_type=jnp.float32).astype(jnp.bfloat16)
    node_cat = jnp.concatenate([nodes, aggregate], axis=1)
    node_pre = jnp.dot(node_cat, node_in_weight, preferred_element_type=jnp.float32) + node_bias
    node_act, node_slope = silu_parts(node_pre)
    node_hidden = node_act.astype(jnp.bfloat16)
    node_pre_grad = (contract(grad_nodes_in, node_out_weight, 1, 1) * node_slope).astype(jnp.bfloat16)
    grad_node_out = contract(node_hidden, grad_nodes_in, 0, 0)
    grad_node_in = contract(node_cat, node_pre_grad, 0, 0)
    node_back = contract(node_pre_grad, node_in_weight, 1, 1)
    grad_aggregate = node_back[:, D:]
    message_grad = (grad_edges_in.astype(jnp.float32) + grad_aggregate[receiver_rows]).astype(jnp.bfloat16)
    edge_pre_grad = (contract(message_grad, edge_out_weight, 1, 1) * edge_slope * live_mask).astype(jnp.bfloat16)
    grad_edge_out = contract(hidden, message_grad, 0, 0)
    grad_edge_in = contract(stacked, edge_pre_grad, 0, 0)
    edge_back = contract(edge_pre_grad, edge_in_weight, 1, 1)
    grad_edges = (grad_edges_in.astype(jnp.float32) + edge_back[:, :D]).astype(jnp.bfloat16)
    node_terms = jax.ops.segment_sum(edge_back[:, D:2 * D], sender_rows, num_segments=NODES)
    node_terms = node_terms + jax.ops.segment_sum(edge_back[:, 2 * D:], receiver_rows, num_segments=NODES)
    grad_nodes = (grad_nodes_in.astype(jnp.float32) + node_back[:, :D] + node_terms).astype(jnp.bfloat16)
    return grad_nodes, grad_edges, grad_edge_in, grad_edge_out, grad_node_in, grad_node_out
```

```python
import functools

import jax
import jax.numpy as jnp
from jax import lax
from jax.experimental import pallas as pl
from jax.experimental.pallas import tpu as pltpu
from jax.sharding import PartitionSpec as P

BF16 = jnp.bfloat16
F32 = jnp.float32
ROWS = 16


def silu_parts(preact):
    logistic = jax.nn.sigmoid(preact)
    return (preact * logistic, logistic * (1.0 + preact * (1.0 - logistic)))


def contract(left_mat, right_mat, left_dim, right_dim):
    return lax.dot_general(
        left_mat,
        right_mat,
        (((left_dim,), (right_dim,)), ((), ())),
        preferred_element_type=F32,
    )


def round_up(value, step):
    return -(-value // step) * step


def halves(value):
    high = value.astype(BF16)
    return high, (value - high.astype(F32)).astype(BF16)


def lanes(parts):
    return jnp.concatenate(parts, axis=1)


def row_onehot(ids_row, count, target=None):
    rows = lax.broadcasted_iota(jnp.int32, (count, ids_row.shape[1]), 0)
    if target is not None:
        rows = target(rows)
    return (rows == ids_row).astype(F32).astype(BF16)


def prepare_kernel(
    nodes, grad_nodes, node_out, edge_out, node_in, edge_bias, node_bias, wanted, outgoing, packed
):
    count = nodes.shape[0]
    share = node_out.shape[0]
    width = nodes.shape[1]
    outgoing[...] = contract(row_onehot(wanted[...], count), nodes[...], 0, 0).astype(BF16)
    for i in range(width // share):
        packed[i * share : (i + 1) * share, :] = edge_out[:, i * share : (i + 1) * share]
    start = width
    packed[start : start + node_in.shape[0], :] = node_in[...]
    start += node_in.shape[0]
    packed[start : start + count, :] = contract(grad_nodes[...], node_out[...], 1, 1).astype(BF16)
    start += count
    edge_high, edge_low = halves(edge_bias[...])
    node_high, node_low = halves(node_bias[...])
    rows = [r.astype(F32) for r in (edge_high, edge_low, node_high, node_low)]
    rows.append(jnp.zeros((ROWS - 4, share), F32))
    packed[start : start + ROWS, :] = jnp.concatenate(rows, axis=0).astype(BF16)


def edge_forward_kernel(slots, *refs):
    chan, counts, senders, receivers, nodes, halo, edges = refs[:7]
    weights = refs[7 : 7 + slots]
    packs = refs[7 + slots : 7 + 2 * slots]
    hidden_own, slope_out, sums_out, rows_out = refs[7 + 2 * slots :]
    local = nodes.shape[0]
    width = nodes.shape[1]
    share = weights[0].shape[1]
    total = edges.shape[0]
    blocks = counts.shape[0]
    block = total // blocks
    remote = halo.shape[0]

    col = pl.multiple_of(chan[0] * (width // slots), width // slots)
    for part in range(3):
        rows_out[part * share : (part + 1) * share, :] = lanes(
            [w[pl.ds(part * width + col, width // slots), :] for w in weights]
        )

    send_hot = row_onehot(senders[...], local)
    far_hot = row_onehot(senders[...], remote, lambda r: r + local)
    recv_hot = row_onehot(receivers[...], local)
    from_send = (
        contract(send_hot, nodes[...], 0, 0) + contract(far_hot, halo[...], 0, 0)
    ).astype(BF16)
    from_recv = contract(recv_hot, nodes[...], 0, 0).astype(BF16)
    stacked = lanes([edges[...], from_send, from_recv])
    bias_at = packs[0].shape[0] - ROWS
    bias = lanes(
        [
            p[bias_at : bias_at + ROWS, :].astype(F32)[0:1, :]
            + p[bias_at : bias_at + ROWS, :].astype(F32)[1:2, :]
            for p in packs
        ]
    )
    weight = lanes([w[...] for w in weights])
    pre = contract(stacked, weight, 1, 0) + bias
    act, slope = silu_parts(pre)
    masks = []
    for b in range(blocks):
        place = lax.broadcasted_iota(jnp.int32, (block, 1), 0)
        masks.append((place < counts[b]).astype(F32))
    live = jnp.concatenate(masks, axis=0)
    hidden = (act * live).astype(BF16)
    hidden_own[...] = hidden[:, :share]
    slope_out[...] = slope * live
    sums_out[...] = contract(recv_hot, hidden, 1, 0).astype(BF16)


def backward_kernel(slots, per_owner, *refs):
    chan, senders, receivers, nodes, halo, edges, grad_nodes, grad_edges = refs[:8]
    hidden_own, slope, sums, edge_rows = refs[8:12]
    packs = refs[12 : 12 + slots]
    edges_out, nodes_out, grads = refs[12 + slots], refs[13 + slots], refs[14 + slots :]
    local = nodes.shape[0]
    width = nodes.shape[1]
    share = hidden_own.shape[1]
    col_share = width // slots
    remote = halo.shape[0]
    owners = remote // per_owner
    col = pl.multiple_of(chan[0] * col_share, col_share)

    edge_out = jnp.concatenate(
        [
            lanes([p[i * share : (i + 1) * share, :] for i in range(width // share)])
            for p in packs
        ],
        axis=0,
    )
    at = width
    node_top = lanes([p[at : at + width, :] for p in packs])
    node_low = lanes([p[at + width : at + 2 * width, :] for p in packs])
    node_rows = lanes([p[pl.ds(at + col, col_share), :] for p in packs])
    at += 2 * width
    pulled = lanes([p[at : at + local, :] for p in packs]).astype(F32)
    at += local
    bias_rows = lanes([p[at : at + ROWS, :] for p in packs]).astype(F32)
    bias = bias_rows[2:3, :] + bias_rows[3:4, :]

    aggregate = contract(sums[...], edge_out, 1, 0).astype(BF16)
    node_pre = contract(nodes[...], node_top, 1, 0) + contract(aggregate, node_low, 1, 0) + bias
    node_act, node_slope = silu_parts(node_pre)
    node_hidden = node_act[:, :share].astype(BF16)
    pre_grad = (pulled * node_slope).astype(BF16)
    back_low = contract(pre_grad, node_low, 1, 1)
    node_own = contract(pre_grad, node_rows, 1, 1)

    recv_hot = row_onehot(receivers[...], local)
    high, low = halves(back_low)
    spread = contract(
        jnp.concatenate([recv_hot, recv_hot], axis=0), jnp.concatenate([high, low], axis=0), 0, 0
    )
    message = (grad_edges[...].astype(F32) + spread).astype(BF16)
    edge_grad = (contract(message, edge_out, 1, 1) * slope[...]).astype(BF16)
    own_grad = edge_grad[:, :share]

    send_hot = row_onehot(senders[...], local)
    far_rows = round_up(per_owner, ROWS)

    def far_id(rows):
        owner, place = rows // far_rows, rows % far_rows
        return jnp.where(place < per_owner, local + owner * per_owner + place, -1)

    if far_rows * owners <= 4 * local:
        far_hot = row_onehot(senders[...], owners * far_rows, far_id)
    else:
        far_hot = row_onehot(senders[...], remote, lambda r: r + local)
    near_hot = row_onehot(senders[...], remote, lambda r: r + local)
    send_sum = contract(send_hot, edge_grad, 1, 0).astype(BF16)
    far_sum = contract(far_hot, edge_grad, 1, 0).astype(BF16)
    recv_sum = contract(recv_hot, edge_grad, 1, 0).astype(BF16)
    near_sum = contract(near_hot, own_grad, 1, 0).astype(BF16)

    row_e = edge_rows[0:share, :]
    row_s = edge_rows[share : 2 * share, :]
    row_r = edge_rows[2 * share : 3 * share, :]
    edges_out[...] = (
        grad_edges[:, pl.ds(col, col_share)].astype(F32) + contract(edge_grad, row_e, 1, 1)
    ).astype(BF16)
    nodes_out[...] = (
        grad_nodes[:, pl.ds(col, col_share)].astype(F32)
        + node_own
        + contract(send_sum, row_s, 1, 1)
        + contract(recv_sum, row_r, 1, 1)
    )
    returned = contract(far_sum, row_s, 1, 1).astype(BF16)

    in_edges = contract(edges[...], own_grad, 0, 0).astype(BF16)
    in_send = (
        contract(nodes[...], send_sum[:, :share], 0, 0) + contract(halo[...], near_sum, 0, 0)
    ).astype(BF16)
    in_recv = contract(nodes[...], recv_sum[:, :share], 0, 0).astype(BF16)
    out_edges = contract(message, hidden_own[...], 0, 0).astype(BF16)
    own_pre = pre_grad[:, :share]
    node_first = contract(nodes[...], own_pre, 0, 0).astype(BF16)
    node_second = contract(aggregate, own_pre, 0, 0).astype(BF16)
    node_outs = contract(grad_nodes[...], node_hidden, 0, 0).astype(BF16)

    groups = (
        jnp.concatenate([in_edges, in_send, in_recv], axis=0),
        out_edges,
        jnp.concatenate([node_first, node_second], axis=0),
        node_outs,
        returned,
    )
    if len(grads) == 1:
        out = grads[0]
        at = 0
        for group in groups:
            size = group.shape[0] // owners
            for q in range(owners):
                out[q, at : at + size, :] = group[q * size : (q + 1) * size, :]
            at += size
    else:
        for ref, group in zip(grads, groups):
            ref[...] = group


def finish_kernel(sizes, per_owner, parts, partial, wanted, *outs):
    grad_nodes, edge_in, edge_out, node_in, node_out = outs
    owners = parts.shape[0]
    at = 0
    totals = []
    for size in sizes[:4]:
        total = parts[0, at : at + size, :].astype(F32)
        for q in range(1, owners):
            total += parts[q, at : at + size, :].astype(F32)
        totals.append(total)
        at += size
    edge_in[...] = totals[0]
    edge_out[...] = totals[1].T
    node_in[...] = totals[2]
    node_out[...] = totals[3].T
    local = partial.shape[0]
    back = jnp.concatenate([parts[q, at : at + sizes[4], :] for q in range(owners)], axis=0)
    rows = lax.broadcasted_iota(jnp.int32, (local, owners * sizes[4]), 0)
    hot = (rows == wanted[...]).astype(F32).astype(BF16)
    grad_nodes[...] = (partial[...] + contract(hot, back, 1, 0)).astype(BF16)


def vmem(count):
    return [pl.BlockSpec(memory_space=pltpu.VMEM)] * count


def smem(count):
    return [pl.BlockSpec(memory_space=pltpu.SMEM)] * count


def call(kernel, name, specs, outs, flops, *args):
    return pl.pallas_call(
        kernel,
        out_shape=outs,
        in_specs=specs,
        out_specs=vmem(len(outs)),
        name=name,
        cost_estimate=pl.CostEstimate(flops=flops, bytes_accessed=4_000_000, transcendentals=0),
    )(*args)


def exchange(value, count, bit):
    return lax.ppermute(value, "chan", [(i, i ^ bit) for i in range(count)])


def gather_slots(value, count):
    slots = [value]
    bit = count // 2
    while bit:
        slots += [exchange(s, count, bit) for s in slots]
        bit //= 2
    return slots


def shape(dims, dtype):
    return jax.ShapeDtypeStruct(dims, dtype)


def body(
    nodes,
    edges,
    grad_nodes_in,
    grad_edges_in,
    edge_in_weight,
    edge_bias,
    edge_out_weight,
    node_in_weight,
    node_bias,
    node_out_weight,
    senders,
    receivers,
    valid_counts,
    send_list,
):
    local, width = nodes.shape
    total = edges.shape[0]
    share = edge_in_weight.shape[1]
    slots = lax.axis_size("chan")
    owners = lax.axis_size("node")
    per_owner = send_list.shape[1]
    remote = owners * per_owner
    chan = lax.axis_index("chan").reshape(1).astype(jnp.int32)
    senders = senders.reshape(1, total)
    receivers = receivers.reshape(1, total)
    wanted = send_list.reshape(1, remote)
    hidden = share * slots

    edge_weights = gather_slots(edge_in_weight, slots)
    pack_rows = width + 2 * width + local + ROWS
    outgoing, packed = call(
        prepare_kernel,
        "prepare",
        vmem(8),
        [shape((remote, width), BF16), shape((pack_rows, share), BF16)],
        1_000_000,
        nodes,
        grad_nodes_in,
        node_out_weight,
        edge_out_weight,
        node_in_weight,
        edge_bias.reshape(1, share),
        node_bias.reshape(1, share),
        wanted,
    )
    halo = lax.all_to_all(outgoing, "node", split_axis=0, concat_axis=0, tiled=True)
    packs = gather_slots(packed, slots)

    hidden_own, slope, sums, edge_rows = call(
        functools.partial(edge_forward_kernel, slots),
        "edge_forward",
        smem(2) + vmem(5 + 2 * slots),
        [
            shape((total, share), BF16),
            shape((total, hidden), F32),
            shape((local, hidden), BF16),
            shape((3 * share, hidden), BF16),
        ],
        700_000_000,
        chan,
        valid_counts,
        senders,
        receivers,
        nodes,
        halo,
        edges,
        *edge_weights,
        *packs,
    )

    far_rows = round_up(per_owner, ROWS)
    sizes = (
        3 * width // owners,
        width // owners,
        2 * width // owners,
        width // owners,
        far_rows,
    )
    direct = all(size % ROWS == 0 for size in sizes) and far_rows * owners <= 4 * local
    if direct:
        grad_shapes = [shape((owners, sum(sizes), share), BF16)]
    else:
        sizes = sizes[:4] + (per_owner,)
        grad_shapes = [shape((owners * size, share), BF16) for size in sizes]
    grad_edges, partial, *grads = call(
        functools.partial(backward_kernel, slots, per_owner),
        "backward",
        smem(1) + vmem(11 + slots),
        [shape((total, share), BF16), shape((local, share), F32), *grad_shapes],
        1_500_000_000,
        chan,
        senders,
        receivers,
        nodes,
        halo,
        edges,
        grad_nodes_in,
        grad_edges_in,
        hidden_own,
        slope,
        sums,
        edge_rows,
        *packs,
    )
    if direct:
        parts = grads[0]
    else:
        parts = jnp.concatenate(
            [g.reshape(owners, size, share) for g, size in zip(grads, sizes)], axis=1
        )
    parts = lax.all_to_all(parts, "node", split_axis=0, concat_axis=0, tiled=True)
    slot_ids = jnp.where(
        jnp.arange(sizes[4]) < per_owner, jnp.pad(send_list, ((0, 0), (0, sizes[4] - per_owner))), -1
    ).reshape(1, owners * sizes[4])
    if direct:
        grad_nodes, rows_edge, cols_edge, rows_node, cols_node = call(
            functools.partial(finish_kernel, sizes, per_owner),
            "finish",
            vmem(3),
            [
                shape((local, share), BF16),
                shape((sizes[0], share), F32),
                shape((share, sizes[1]), F32),
                shape((sizes[2], share), F32),
                shape((share, sizes[3]), F32),
            ],
            10_000_000,
            parts,
            partial,
            slot_ids,
        )
    else:
        pieces = []
        at = 0
        for size in sizes[:4]:
            pieces.append(jnp.sum(parts[:, at : at + size].astype(F32), axis=0))
            at += size
        rows_edge, cols_edge, rows_node, cols_node = pieces
        cols_edge, cols_node = cols_edge.T, cols_node.T
        back = parts[:, at:].astype(F32).reshape(remote, share)
        grad_nodes = (
            partial + jax.ops.segment_sum(back, send_list.reshape(-1), num_segments=local)
        ).astype(BF16)
    return (grad_nodes, grad_edges, rows_edge, cols_edge, rows_node, cols_node)


def solution(mesh):
    in_specs = (
        P("node", None),
        P("node", None),
        P("node", None),
        P("node", None),
        P(None, "chan"),
        P("chan"),
        P("chan", None),
        P(None, "chan"),
        P("chan"),
        P("chan", None),
        P("node"),
        P("node"),
        P("node"),
        P("node", None),
    )
    out_specs = (
        P("node", "chan"),
        P("node", "chan"),
        P("node", "chan"),
        P("chan", "node"),
        P("node", "chan"),
        P("chan", "node"),
    )
    return jax.shard_map(body, mesh=mesh, in_specs=in_specs, out_specs=out_specs, check_vma=False)
```
